32 devices in a mesh: site: 2 (over core), replica: 4 (over z), model: 4 (over y, x).
Axes of the slice: x: 2, y: 2, z: 4, core: 2. Of those that a mesh axis runs over, the one named last changes fastest.
Arguments:
- partial_query: bfloat16 [8, 1024, 1024], P(('site', 'replica'), None, 'model'), parts along dimension 0, may hold values from -4 to 4
- partial_key: bfloat16 [8, 1024, 1024], P(('site', 'replica'), None, 'model'), parts along dimension 0, may hold values from -4 to 4
- partial_value: bfloat16 [8, 1024, 1024], P(('site', 'replica'), None, 'model'), parts along dimension 0, may hold values from -4 to 4
- partial_mixed: bfloat16 [8, 1024, 1024], P(('site', 'replica'), 'model'), parts along dimension 0, may hold values from -4 to 4
- partial_norm: bfloat16 [8, 1024], P(('site', 'replica')), parts along dimension 0, may hold values from -8 to 8
- master_query: float32 [2048, 1024], P(('site', 'replica'), 'model'), parts along dimension 0, may hold values from -0.1875 to 0.1875
- master_key: float32 [2048, 1024], P(('site', 'replica'), 'model'), parts along dimension 0, may hold values from -0.1875 to 0.1875
- master_value: float32 [2048, 1024], P(('site', 'replica'), 'model'), parts along dimension 0, may hold values from -0.1875 to 0.1875
- master_mixed: float32 [2048, 1024], P(('site', 'model'), 'replica'), parts along dimension 0, may hold values from -0.1875 to 0.1875
- master_norm: float32 [2048], P(('site', 'replica')), parts along dimension 0, may hold values from 0.25 to 1.75
- memory_query: float32 [2048, 1024], P(('site', 'replica'), 'model'), parts along dimension 0, may hold values from 0.05 to 0.8
- memory_key: float32 [2048, 1024], P(('site', 'replica'), 'model'), parts along dimension 0, may hold values from 0.05 to 0.8
- memory_value: float32 [2048, 1024], P(('site', 'replica'), 'model'), parts along dimension 0, may hold values from 0.05 to 0.8
- memory_mixed: float32 [2048, 1024], P(('site', 'model'), 'replica'), parts along dimension 0, may hold values from 0.05 to 0.8
- memory_norm: float32 [2048], P(('site', 'replica')), parts along dimension 0, may hold values from 0.05 to 0.8
Outputs:
- compute_query: bfloat16 [2048, 1024], P('site', 'model'), parts along dimension 0
- compute_key: bfloat16 [2048, 1024], P('site', 'model'), parts along dimension 0
- compute_value: bfloat16 [2048, 1024], P('site', 'model'), parts along dimension 0
- compute_mixed: bfloat16 [2048, 1024], P(('site', 'model')), parts along dimension 0
- compute_norm: bfloat16 [2048], P('site'), parts along dimension 0
- stepped_query: float32 [2048, 1024], P(('site', 'replica'), 'model'), parts along dimension 0
- stepped_key: float32 [2048, 1024], P(('site', 'replica'), 'model'), parts along dimension 0
- stepped_value: float32 [2048, 1024], P(('site', 'replica'), 'model'), parts along dimension 0
- stepped_mixed: float32 [2048, 1024], P(('site', 'model'), 'replica'), parts along dimension 0
- stepped_norm: float32 [2048], P(('site', 'replica')), parts along dimension 0
- state_new_query: float32 [2048, 1024], P(('site', 'replica'), 'model'), parts along dimension 0
- state_new_key: float32 [2048, 1024], P(('site', 'replica'), 'model'), parts along dimension 0
- state_new_value: float32 [2048, 1024], P(('site', 'replica'), 'model'), parts along dimension 0
- state_new_mixed: float32 [2048, 1024], P(('site', 'model'), 'replica'), parts along dimension 0
- state_new_norm: float32 [2048], P(('site', 'replica')), parts along dimension 0
The draws below stay inside these ranges and needn't reach their ends.
There are 2 independent parts, one for each index of `site`. The reference program is written for one: setup_inputs(seed, part) draws one part's arguments, and reference() takes and returns one part's arrays. A program takes and returns all parts, laid end to end along the dimension named above; each array names one. Nothing has to cross between parts.
All inputs are finite; a program needn't handle non-finite values.
Results may differ from the reference program's by a relative error of at most 0.001.
Values may be sent and summed in bfloat16 or wider, within the bound.
A program may use at most 64 MiB of HBM per device.

```python
import jax
import jax.numpy as jnp
from jax import lax

WIDTH = 1024
ATTN = 1024
REPLICAS = 4


def spiked(values, rng, source, target, blocks, factor):
    def block_of(axis_at):
        return (jnp.arange(values.shape[axis_at]) // (values.shape[axis_at] // blocks)).reshape((-1,) + (1,) * (values.ndim - 1 - axis_at))

    one_side = jax.random.permutation(rng, blocks)[block_of(target)]
    second = (block_of(target) + blocks // 2) % blocks
    return jnp.where((block_of(source) == one_side) | (block_of(source) == second), factor * values, values)


def level_of(key, dims, cuts, least, largest):
    def one(dim, blocks):
        steps = jax.random.uniform(jax.random.fold_in(jax.random.fold_in(key, 6), dim), (blocks,), jnp.float32, least / len(cuts), largest / len(cuts))
        return jnp.repeat(jnp.exp(steps), dims[dim] // blocks).reshape((-1,) + (1,) * (len(dims) - dim - 1))

    gain = one(*cuts[0])
    for cut in cuts[1:]:
        gain = gain * one(*cut)
    return gain


def centred(own_key, dims, spread, bound, pieces=(), kind=jnp.bfloat16):
    drawn = spread * jax.random.normal(own_key, dims, jnp.float32)
    if pieces:
        drawn = drawn * level_of(own_key, dims, pieces, -0.22, 0.18)
    return jnp.clip(drawn, -bound, bound).astype(kind)


def bell_draw_with(stream_key, extent, spread, reach, shards, heavy, dtype=jnp.bfloat16):
    entries = spread * jax.random.normal(stream_key, extent, jnp.float32)
    if shards:
        entries = entries * level_of(stream_key, extent, shards, -0.22, 0.18)
    return jnp.clip(spiked(entries, jax.random.fold_in(stream_key, 3), *heavy), -reach, reach).astype(dtype)


def setup_inputs(seed: int = 0, part: int = 0) -> dict:
    splits = jax.random.split(jax.random.key(seed), 16)
    own_keys = jax.random.split(jax.random.fold_in(splits[15], part), 16)
    partial_query = bell_draw_with(own_keys[0], (REPLICAS, WIDTH, ATTN), 0.5, 4.0, ((0, 4), (2, 4)), (0, 1, 4, 2.0))
    partial_key = bell_draw_with(own_keys[1], (REPLICAS, WIDTH, ATTN), 0.5, 4.0, ((0, 4), (2, 4)), (0, 1, 4, 2.0))
    partial_value = bell_draw_with(own_keys[2], (REPLICAS, WIDTH, ATTN), 0.5, 4.0, ((0, 4), (2, 4)), (0, 1, 4, 2.0))
    partial_mixed = bell_draw_with(own_keys[3], (REPLICAS, ATTN, WIDTH), 0.5, 4.0, ((0, 4), (1, 4)), (0, 2, 4, 2.0))
    partial_norm = bell_draw_with(own_keys[4], (REPLICAS, WIDTH), 1.0, 8.0, ((0, 4),), (0, 1, 4, 2.0))
    master_query = centred(own_keys[5], (WIDTH, ATTN), WIDTH ** -0.5, 0.1875, ((0, 4), (1, 4)), jnp.float32)
    master_key = centred(own_keys[6], (WIDTH, ATTN), WIDTH ** -0.5, 0.1875, ((0, 4), (1, 4)), jnp.float32)
    master_value = centred(own_keys[7], (WIDTH, ATTN), WIDTH ** -0.5, 0.1875, ((0, 4), (1, 4)), jnp.float32)
    master_mixed = centred(own_keys[8], (ATTN, WIDTH), ATTN ** -0.5, 0.1875, ((0, 4), (1, 4)), jnp.float32)
    master_norm = jnp.clip(1.0 + 0.15 * jax.random.normal(own_keys[9], (WIDTH,), jnp.float32), 0.25, 1.75)
    memory_query = jnp.clip(0.05 + 0.75 * jax.random.uniform(own_keys[10], (WIDTH, ATTN), jnp.float32) ** level_of(own_keys[10], (WIDTH, ATTN), ((0, 4), (1, 4)), -0.2, 0.2), 0.05, 0.8)
    memory_key = jnp.clip(0.05 + 0.75 * jax.random.uniform(own_keys[11], (WIDTH, ATTN), jnp.float32) ** level_of(own_keys[11], (WIDTH, ATTN), ((0, 4), (1, 4)), -0.2, 0.2), 0.05, 0.8)
    memory_value = jnp.clip(0.05 + 0.75 * jax.random.uniform(own_keys[12], (WIDTH, ATTN), jnp.float32) ** level_of(own_keys[12], (WIDTH, ATTN), ((0, 4), (1, 4)), -0.2, 0.2), 0.05, 0.8)
    memory_mixed = jnp.clip(0.05 + 0.75 * jax.random.uniform(own_keys[13], (ATTN, WIDTH), jnp.float32) ** level_of(own_keys[13], (ATTN, WIDTH), ((0, 4), (1, 4)), -0.2, 0.2), 0.05, 0.8)
    memory_norm = jnp.clip(0.05 + 0.75 * jax.random.uniform(own_keys[14], (WIDTH,), jnp.float32) ** level_of(own_keys[14], (WIDTH,), ((0, 4),), -0.2, 0.2), 0.05, 0.8)
    return {"partial_query": partial_query, "partial_key": partial_key, "partial_value": partial_value, "partial_mixed": partial_mixed, "partial_norm": partial_norm, "master_query": master_query, "master_key": master_key, "master_value": master_value, "master_mixed": master_mixed, "master_norm": master_norm, "memory_query": memory_query, "memory_key": memory_key, "memory_value": memory_value, "memory_mixed": memory_mixed, "memory_norm": memory_norm}


learn_rate = 0.05
hold_rate = 0.7

def reference(partial_query, partial_key, partial_value, partial_mixed, partial_norm, master_query, master_key, master_value, master_mixed, master_norm, memory_query, memory_key, memory_value, memory_mixed, memory_norm):
    mean_query = lax.optimization_barrier(jnp.sum(partial_query.astype(jnp.float32), axis=0)) * REPLICAS ** (-0.5)
    mean_key = lax.optimization_barrier(jnp.sum(partial_key.astype(jnp.float32), axis=0)) * REPLICAS ** (-0.5)
    mean_value = lax.optimization_barrier(jnp.sum(partial_value.astype(jnp.float32), axis=0)) * REPLICAS ** (-0.5)
    mean_mixed = lax.optimization_barrier(jnp.sum(partial_mixed.astype(jnp.float32), axis=0)) * REPLICAS ** (-0.5)
    mean_norm = lax.optimization_barrier(jnp.sum(partial_norm.astype(jnp.float32), axis=0)) * REPLICAS ** (-0.5)
    state_new_query = hold_rate * memory_query + (1.0 - hold_rate) * mean_query * mean_query
    stepped_query = master_query - learn_rate * mean_query * lax.rsqrt(state_new_query + 1e-06)
    state_new_key = hold_rate * memory_key + (1.0 - hold_rate) * mean_key * mean_key
    stepped_key = master_key - learn_rate * mean_key * lax.rsqrt(state_new_key + 1e-06)
    state_new_value = hold_rate * memory_value + (1.0 - hold_rate) * mean_value * mean_value
    stepped_value = master_value - learn_rate * mean_value * lax.rsqrt(state_new_value + 1e-06)
    state_new_mixed = hold_rate * memory_mixed + (1.0 - hold_rate) * mean_mixed * mean_mixed
    stepped_mixed = master_mixed - learn_rate * mean_mixed * lax.rsqrt(state_new_mixed + 1e-06)
    state_new_norm = hold_rate * memory_norm + (1.0 - hold_rate) * mean_norm * mean_norm
    stepped_norm = master_norm - learn_rate * mean_norm * lax.rsqrt(state_new_norm + 1e-06)
    compute_query = stepped_query.astype(jnp.bfloat16)
    compute_key = stepped_key.astype(jnp.bfloat16)
    compute_value = stepped_value.astype(jnp.bfloat16)
    compute_mixed = stepped_mixed.astype(jnp.bfloat16)
    compute_norm = stepped_norm.astype(jnp.bfloat16)
    return (compute_query, compute_key, compute_value, compute_mixed, compute_norm, stepped_query, stepped_key, stepped_value, stepped_mixed, stepped_norm, state_new_query, state_new_key, state_new_value, state_new_mixed, state_new_norm)
```

```python
import functools

import jax
import jax.numpy as jnp
from jax import lax
from jax.experimental import pallas as pl
from jax.experimental.pallas import tpu as pltpu
from jax.sharding import PartitionSpec as P

learn_rate = 0.05
hold_rate = 0.7
HALVES = 2
MESH = pl.DeviceIdType.MESH
LINK = jnp.bfloat16
MATRICES = 4
LIMIT = 4.0
TOP = 120.0


def update(mean, master, memory):
    state = hold_rate * memory + (1.0 - hold_rate) * mean * mean
    return master - learn_rate * mean * lax.rsqrt(state + 1e-06), state


def encode(value, gain):
    size = jnp.exp2(jnp.abs(value) * gain - TOP)
    return jnp.where(value < 0, -size, size).astype(LINK)


def decode(code, step):
    code = code.astype(jnp.float32)
    size = (jnp.log2(jnp.abs(code)) + TOP) * step
    return jnp.where(code < 0, -size, size)


def kernel(n, halves, *refs):
    T = MATRICES
    (partial, master, memory) = refs[0:T], refs[T : 2 * T], refs[2 * T : 3 * T]
    norm_in = refs[3 * T]
    at = 3 * T + 1
    compute, stepped, state = refs[at : at + T], refs[at + T : at + 2 * T], refs[at + 2 * T : at + 3 * T]
    compute_norm, stepped_norm, state_norm = refs[at + 3 * T : at + 3 * T + 3]
    (
        tall, wide, master_v, memory_v, send_v, recv_v, acc, step_v, state_v, tall_g, wide_g, norm_v,
        load_sem, rs_send, rs_recv, ag_send, ag_recv, norm_send, norm_recv, out_sem, gather_sem,
    ) = refs[at + 3 * T + 3 :]
    me = lax.axis_index("replica")
    rows, cols = master[0].shape
    part = rows // halves
    rate = n ** (-0.5)

    def spot(plane, planes_wide, t, s, h):
        if t < T - 1:
            top = pl.multiple_of(s * rows + h * part, part)
            return plane.at[t, pl.ds(top, part), :]
        return planes_wide.at[pl.ds(h * part, part), pl.ds(pl.multiple_of(s * cols, cols), cols)]

    loads = []
    for t in range(T):
        loads.append(
            (
                pltpu.make_async_copy(partial[t], tall.at[t] if t < T - 1 else wide, load_sem.at[0, t]),
                pltpu.make_async_copy(master[t], master_v.at[t], load_sem.at[1, t]),
                pltpu.make_async_copy(memory[t], memory_v.at[t], load_sem.at[2, t]),
            )
        )
    for t in range(T):
        loads[t][0].start()
    for t in range(T):
        loads[t][1].start()
        loads[t][2].start()

    barrier = pltpu.get_barrier_semaphore()
    for d in range(1, n):
        pl.semaphore_signal(
            barrier, inc=1, device_id={"replica": lax.rem(me + d, n)}, device_id_type=MESH
        )
    pl.semaphore_wait(barrier, n - 1)

    def norm_copy(d):
        return pltpu.make_async_remote_copy(
            src_ref=norm_in,
            dst_ref=norm_v.at[d - 1],
            send_sem=norm_send.at[d - 1],
            recv_sem=norm_recv.at[d - 1],
            device_id={"replica": lax.rem(me + d, n)},
            device_id_type=MESH,
        )

    def sum_copy(way, c, s, source=None):
        return pltpu.make_async_remote_copy(
            src_ref=send_v.at[way, c, s] if source is None else source,
            dst_ref=recv_v.at[way, c, s],
            send_sem=rs_send.at[way, c, s],
            recv_sem=rs_recv.at[way, c, s],
            device_id={"replica": me + 1 - 2 * way},
            device_id_type=MESH,
        )

    def share_copy(way, c, s):
        t, h = c // halves, c % halves
        place = spot(tall_g, wide_g, t, s, h)
        return pltpu.make_async_remote_copy(
            src_ref=place,
            dst_ref=place,
            send_sem=ag_send.at[way, c, s],
            recv_sem=ag_recv.at[way, c, s],
            device_id={"replica": me + 1 - 2 * way},
            device_id_type=MESH,
        )

    def terms(way):
        return me + 1 if way == 0 else n - me

    def gain(way):
        return (2 * TOP / LIMIT) / terms(way).astype(jnp.float32)

    def arrived(way, c, s):
        step = (terms(way) - 1).astype(jnp.float32) * (LIMIT / (2 * TOP))
        code = recv_v[way, c, s]
        return jnp.where(terms(way) == 2, code.astype(jnp.float32), decode(code, step))

    def behind(way):
        return me > 0 if way == 0 else me < n - 1

    def ahead(way, d):
        return me + d < n if way == 0 else me - d >= 0

    def sums(c):
        t, h = c // halves, c % halves
        if h == 0:
            loads[t][0].wait()
        for d in range(n - 1, 0, -1):
            for way in range(2):
                s = me + d if way == 0 else me - d

                @pl.when(jnp.logical_and(ahead(way, d), jnp.logical_not(behind(way))))
                def _():
                    sum_copy(way, c, s, spot(tall, wide, t, s, h)).start()

                @pl.when(jnp.logical_and(ahead(way, d), behind(way)))
                def _():
                    own = spot(tall, wide, t, s, h)[...].astype(jnp.float32)
                    sum_copy(way, c, s).wait_recv()
                    send_v[way, c, s] = encode(own + arrived(way, c, s), gain(way))
                    sum_copy(way, c, s).start()

    def finish(c):
        t, h = c // halves, c % halves
        if h == 0:
            loads[t][1].wait()
            loads[t][2].wait()
        acc[...] = spot(tall, wide, t, me, h)[...].astype(jnp.float32)
        for way in range(2):

            @pl.when(behind(way))
            def _():
                sum_copy(way, c, me).wait_recv()
                acc[...] += arrived(way, c, me)

        band = pl.ds(h * part, part)
        new, held = update(acc[...] * rate, master_v[t, band, :], memory_v[t, band, :])
        spot(tall_g, wide_g, t, me, h)[...] = new.astype(jnp.bfloat16)
        for way in range(2):

            @pl.when(ahead(way, 1))
            def _():
                share_copy(way, c, me).start()

        step_v[t, band, :] = new
        state_v[t, band, :] = held
        if h == halves - 1:
            pltpu.make_async_copy(step_v.at[t], stepped[t], out_sem.at[0, t]).start()
            pltpu.make_async_copy(state_v.at[t], state[t], out_sem.at[1, t]).start()

    def gathered_copy(t):
        return pltpu.make_async_copy(tall_g.at[t] if t < T - 1 else wide_g, compute[t], gather_sem.at[t])

    def forward(c):
        t, h = c // halves, c % halves
        for d in range(1, n):
            for way in range(2):
                s = me - d if way == 0 else me + d
                there = s >= 0 if way == 0 else s < n

                @pl.when(there)
                def _():
                    share_copy(way, c, s).wait_recv()

                @pl.when(jnp.logical_and(there, ahead(way, 1)))
                def _():
                    share_copy(way, c, s).start()

        if h == halves - 1:
            gathered_copy(t).start()

    count = T * halves
    for step in range(count + 2):
        if step < count:
            sums(step)
        if step == 0:
            for d in range(1, n):
                norm_copy(d).start()
        if 1 <= step <= count:
            finish(step - 1)
        if step >= 2:
            forward(step - 2)

    whole = norm_in.shape[1] - 2 * cols
    for d in range(1, n):
        norm_copy(d).wait()
    mean_norm = norm_in[:, :whole]
    for d in range(1, n):
        mean_norm = mean_norm + norm_v[d - 1][:, :whole]
    mean_norm = mean_norm * rate
    for s in range(n):
        mean_s = mean_norm[:, s * cols : (s + 1) * cols]

        @pl.when(me == s)
        def _():
            new, held = update(mean_s, norm_in[:, whole : whole + cols], norm_in[:, whole + cols :])
            stepped_norm[...] = new
            state_norm[...] = held
            compute_norm[:, s * cols : (s + 1) * cols] = new.astype(jnp.bfloat16)

        @pl.when(me != s)
        def _():
            slot = lax.rem(me - s + n, n) - 1
            new, held = update(
                mean_s, norm_v[slot, :, whole : whole + cols], norm_v[slot, :, whole + cols :]
            )
            compute_norm[:, s * cols : (s + 1) * cols] = new.astype(jnp.bfloat16)

    for c in range(count):
        for d in range(1, n):
            for way in range(2):

                @pl.when(ahead(way, d))
                def _():
                    sum_copy(way, c, me + d if way == 0 else me - d).wait_send()

        for d in range(n):
            for way in range(2):
                s = me - d if way == 0 else me + d

                @pl.when(jnp.logical_and(s >= 0 if way == 0 else s < n, ahead(way, 1)))
                def _():
                    share_copy(way, c, s).wait_send()

    for t in range(T):
        pltpu.make_async_copy(step_v.at[t], stepped[t], out_sem.at[0, t]).wait()
        pltpu.make_async_copy(state_v.at[t], state[t], out_sem.at[1, t]).wait()
        gathered_copy(t).wait()


def line(n, partials, masters, memories, partial_norm, master_norm, memory_norm):
    T, halves = MATRICES, HALVES
    rows, cols = masters[0].shape
    part = rows // halves
    count = T * halves
    whole = partial_norm.shape[1]
    norm_in = jnp.concatenate(
        [partial_norm.astype(jnp.float32), master_norm[None], memory_norm[None]], axis=1
    )
    f32, bf16 = jnp.float32, jnp.bfloat16
    anywhere = pl.BlockSpec(memory_space=pl.ANY)
    inside = pl.BlockSpec(memory_space=pltpu.VMEM)
    share = jax.ShapeDtypeStruct((rows, cols), f32)
    dma = pltpu.SemaphoreType.DMA
    out = pl.pallas_call(
        functools.partial(kernel, n, halves),
        out_shape=[jax.ShapeDtypeStruct(p.shape, bf16) for p in partials]
        + [share] * (2 * T)
        + [jax.ShapeDtypeStruct((1, whole), bf16)]
        + [jax.ShapeDtypeStruct((1, cols), f32)] * 2,
        in_specs=[anywhere] * (3 * T) + [inside],
        out_specs=[anywhere] * (3 * T) + [inside] * 3,
        scratch_shapes=[
            pltpu.VMEM((T - 1, n * rows, cols), bf16),
            pltpu.VMEM((rows, n * cols), bf16),
            pltpu.VMEM((T, rows, cols), f32),
            pltpu.VMEM((T, rows, cols), f32),
            pltpu.VMEM((2, count, n, part, cols), LINK),
            pltpu.VMEM((2, count, n, part, cols), LINK),
            pltpu.VMEM((part, cols), f32),
            pltpu.VMEM((T, rows, cols), f32),
            pltpu.VMEM((T, rows, cols), f32),
            pltpu.VMEM((T - 1, n * rows, cols), bf16),
            pltpu.VMEM((rows, n * cols), bf16),
            pltpu.VMEM((n - 1, 1, whole + 2 * cols), f32),
            dma((3, T)),
            dma((2, count, n)),
            dma((2, count, n)),
            dma((2, count, n)),
            dma((2, count, n)),
            dma((n - 1,)),
            dma((n - 1,)),
            dma((2, T)),
            dma((T,)),
        ],
        compiler_params=pltpu.CompilerParams(collective_id=0, has_side_effects=True),
        name="line_step",
    )(*partials, *masters, *memories, norm_in)
    compute, stepped, state = out[:T], out[T : 2 * T], out[2 * T : 3 * T]
    compute_norm, stepped_norm, state_norm = out[3 * T :]
    return (*compute, compute_norm[0], *stepped, stepped_norm[0], *state, state_norm[0])


def plain(n, partials, masters, memories, partial_norm, master_norm, memory_norm):
    rate = n ** (-0.5)
    axes = (0, 0, 0, 1)
    compute, stepped, state = [], [], []
    for p, master, memory, axis in zip(partials, masters, memories, axes):
        total = lax.psum_scatter(
            p.astype(jnp.float32), "replica", scatter_dimension=axis, tiled=True
        )
        new, held = update(total * rate, master, memory)
        stepped.append(new)
        state.append(held)
    whole = lax.psum(partial_norm[0].astype(jnp.float32), "replica")
    size = master_norm.shape[0]
    mean = lax.dynamic_slice_in_dim(whole, lax.axis_index("replica") * size, size) * rate
    new, held = update(mean, master_norm, memory_norm)
    stepped.append(new)
    state.append(held)
    for new, axis in zip(stepped, axes + (0,)):
        compute.append(lax.all_gather(new.astype(jnp.bfloat16), "replica", axis=axis, tiled=True))
    return (*compute, *stepped, *state)


def body(*args):
    partials = [p[0] for p in args[:4]]
    partial_norm = args[4]
    masters, master_norm = args[5:9], args[9]
    memories, memory_norm = args[10:14], args[14]
    n = lax.axis_size("replica")
    shapes = {m.shape for m in masters}
    rows, cols = masters[0].shape
    fits = (
        1 < n <= 4
        and len(shapes) == 1
        and rows % (32 * HALVES) == 0
        and cols % 128 == 0
        and master_norm.shape[0] == cols
    )
    form = line if fits else plain
    return form(n, partials, masters, memories, partial_norm, master_norm, memory_norm)


def solution(mesh):
    tall = P(("site", "replica"), None, "model")
    share, flat = P(("site", "replica"), "model"), P(("site", "replica"))
    wide = P(("site", "model"), "replica")
    shares = (share, share, share, wide, flat)
    return jax.shard_map(
        body,
        mesh=mesh,
        in_specs=(
            tall,
            tall,
            tall,
            P(("site", "replica"), "model", None),
            P(("site", "replica"), None),
            *shares,
            *shares,
        ),
        out_specs=(
            P("site", "model"),
            P("site", "model"),
            P("site", "model"),
            P(("site", "model"), None),
            P("site"),
            *shares,
            *shares,
        ),
        check_vma=False,
    )
```

```python
import functools

import jax
import jax.numpy as jnp
from jax import lax
from jax.experimental import pallas as pl
from jax.experimental.pallas import tpu as pltpu
from jax.sharding import PartitionSpec as P

learn_rate = 0.05
hold_rate = 0.7
HALVES = 2
GAP = 1
LEAD = 2
MESH = pl.DeviceIdType.MESH
LINK = jnp.bfloat16
MATRICES = 4
LIMIT = 4.0
TOP = 120.0


def update(mean, master, memory):
    state = hold_rate * memory + (1.0 - hold_rate) * mean * mean
    return master - learn_rate * mean * lax.rsqrt(state + 1e-06), state


def encode(value, gain):
    size = jnp.exp2(jnp.abs(value) * gain - TOP)
    return jnp.where(value < 0, -size, size).astype(LINK)


def decode(code, step):
    code = code.astype(jnp.float32)
    size = (jnp.log2(jnp.abs(code)) + TOP) * step
    return jnp.where(code < 0, -size, size)


def kernel(n, halves, *refs):
    T = MATRICES
    (partial, master, memory) = refs[0:T], refs[T : 2 * T], refs[2 * T : 3 * T]
    norm_in = refs[3 * T]
    at = 3 * T + 1
    compute, stepped, state = refs[at : at + T], refs[at + T : at + 2 * T], refs[at + 2 * T : at + 3 * T]
    compute_norm, stepped_norm, state_norm = refs[at + 3 * T : at + 3 * T + 3]
    (
        tall, master_v, memory_v, send_v, recv_v, acc, step_v, state_v, tall_g, norm_v, load_sem,
        held_sem, rs_send, rs_recv, ag_send, ag_recv, norm_send, norm_recv, out_sem, gather_sem,
    ) = refs[at + 3 * T + 3 :]
    me = lax.axis_index("replica")
    rows, cols = master[0].shape
    part = rows // halves
    rate = n ** (-0.5)

    def spot(plane, c, s):
        top = pl.multiple_of(s * rows + (c % halves) * part, part)
        return plane.at[c // halves, pl.ds(top, part), :]

    def laid(plane, whole, t, out, sem):
        if t < T - 1:
            pairs = [(whole, plane.at[t])]
        else:
            pairs = [
                (whole.at[:, s * cols : (s + 1) * cols], plane.at[t, s * rows : (s + 1) * rows])
                for s in range(n)
            ]
        return [
            pltpu.make_async_copy(*(pair[::-1] if out else pair), sem.at[t, i])
            for i, pair in enumerate(pairs)
        ]

    loads = [laid(tall, partial[t], t, False, load_sem) for t in range(T)]
    held = [
        pltpu.make_async_copy(source[t], target.at[t], held_sem.at[i, t])
        for i, (source, target) in enumerate(((master, master_v), (memory, memory_v)))
        for t in range(T)
    ]
    for copy in sum(loads, []) + held:
        copy.start()

    barrier = pltpu.get_barrier_semaphore()
    for d in range(1, n):
        pl.semaphore_signal(
            barrier, inc=1, device_id={"replica": lax.rem(me + d, n)}, device_id_type=MESH
        )
    pl.semaphore_wait(barrier, n - 1)

    def norm_copy(d):
        return pltpu.make_async_remote_copy(
            src_ref=norm_in,
            dst_ref=norm_v.at[d - 1],
            send_sem=norm_send.at[d - 1],
            recv_sem=norm_recv.at[d - 1],
            device_id={"replica": lax.rem(me + d, n)},
            device_id_type=MESH,
        )

    def sum_copy(way, c, s, source=None):
        return pltpu.make_async_remote_copy(
            src_ref=send_v.at[way, c, s] if source is None else source,
            dst_ref=recv_v.at[way, c, s],
            send_sem=rs_send.at[way, c, s],
            recv_sem=rs_recv.at[way, c, s],
            device_id={"replica": me + 1 - 2 * way},
            device_id_type=MESH,
        )

    def share_copy(way, c, s):
        place = spot(tall_g, c, s)
        return pltpu.make_async_remote_copy(
            src_ref=place,
            dst_ref=place,
            send_sem=ag_send.at[way, c, s],
            recv_sem=ag_recv.at[way, c, s],
            device_id={"replica": me + 1 - 2 * way},
            device_id_type=MESH,
        )

    def terms(way):
        return me + 1 if way == 0 else n - me

    def gain(way):
        return (2 * TOP / LIMIT) / terms(way).astype(jnp.float32)

    def arrived(way, c, s):
        step = (terms(way) - 1).astype(jnp.float32) * (LIMIT / (2 * TOP))
        code = recv_v[way, c, s]
        return jnp.where(terms(way) == 2, code.astype(jnp.float32), decode(code, step))

    def behind(way):
        return me > 0 if way == 0 else me < n - 1

    def ahead(way, d):
        return me + d < n if way == 0 else me - d >= 0

    def either(way, d):
        return me + d if way == 0 else me - d

    def inner(c):
        return jnp.logical_and(c >= 0, c < count)

    def raw(c):
        for d in range(n - 1, 0, -1):
            for way in range(2):

                @pl.when(jnp.logical_and(ahead(way, d), jnp.logical_not(behind(way))))
                def _():
                    sum_copy(way, c, either(way, d), spot(tall, c, either(way, d))).start()

    def sums(way, c):
        for d in range(n - 1, 0, -1):
            s = either(way, d)

            @pl.when(jnp.logical_and(inner(c), jnp.logical_and(ahead(way, d), behind(way))))
            def _():
                own = spot(tall, c, s)[...].astype(jnp.float32)
                sum_copy(way, c, s).wait_recv()
                send_v[way, c, s] = encode(own + arrived(way, c, s), gain(way))
                sum_copy(way, c, s).start()

    def finish(c):
        acc[...] = spot(tall, c, me)[...].astype(jnp.float32)
        for way in range(2):

            @pl.when(behind(way))
            def _():
                sum_copy(way, c, me).wait_recv()
                acc[...] += arrived(way, c, me)

        t, band = c // halves, pl.ds(pl.multiple_of((c % halves) * part, part), part)
        new, held = update(acc[...] * rate, master_v[t, band, :], memory_v[t, band, :])
        spot(tall_g, c, me)[...] = new.astype(jnp.bfloat16)
        for way in range(2):

            @pl.when(ahead(way, 1))
            def _():
                share_copy(way, c, me).start()

        step_v[t, band, :] = new
        state_v[t, band, :] = held

    def forward(way, d, c, s):
        @pl.when(jnp.logical_and(inner(c), jnp.logical_and(s >= 0, s < n)))
        def _():
            share_copy(way, c, s).wait_recv()

            @pl.when(ahead(way, 1))
            def _():
                share_copy(way, c, s).start()

    def depth(s):
        return jnp.maximum(s, n - 1 - s)

    def step(at, carry):
        @pl.when(at + LEAD < count)
        def _():
            raw(at + LEAD)

        for way in range(2):
            sums(way, at - GAP * (terms(way) - 1))
        c = at - GAP * depth(me)

        @pl.when(inner(c))
        def _():
            finish(c)

        for d in range(1, n):
            for way in range(2):
                s = either(1 - way, d)
                forward(way, d, at - GAP * (depth(s) + d), s)
        return carry

    count = T * halves
    for t in range(T):
        for copy in loads[t]:
            copy.wait()
        for c in range(t * halves, (t + 1) * halves):
            if c < LEAD:
                raw(c)
    for d in range(1, n):
        norm_copy(d).start()
    for copy in held:
        copy.wait()

    outs = [
        pltpu.make_async_copy(source.at[t], target[t], out_sem.at[i, t])
        for t in range(T)
        for i, (source, target) in enumerate(((step_v, stepped), (state_v, state)))
    ]
    gathered = [laid(tall_g, compute[t], t, True, gather_sem) for t in range(T)]
    tasks = sorted(
        [(t * halves + halves - 1 + GAP * (n - 1), outs[2 * t : 2 * t + 2]) for t in range(T)]
        + [(t * halves + halves - 1 + 2 * GAP * (n - 1), gathered[t]) for t in range(T)],
        key=lambda task: task[0],
    )
    reached = 0
    for last, copies in tasks:
        if last >= reached:
            lax.fori_loop(reached, last + 1, step, 0)
            reached = last + 1
        for copy in copies:
            copy.start()

    whole = norm_in.shape[1] - 2 * cols
    for d in range(1, n):
        norm_copy(d).wait()
    mean_norm = norm_in[:, :whole]
    for d in range(1, n):
        mean_norm = mean_norm + norm_v[d - 1][:, :whole]
    mean_norm = mean_norm * rate
    for s in range(n):
        mean_s = mean_norm[:, s * cols : (s + 1) * cols]

        @pl.when(me == s)
        def _():
            new, held = update(mean_s, norm_in[:, whole : whole + cols], norm_in[:, whole + cols :])
            stepped_norm[...] = new
            state_norm[...] = held
            compute_norm[:, s * cols : (s + 1) * cols] = new.astype(jnp.bfloat16)

        @pl.when(me != s)
        def _():
            slot = lax.rem(me - s + n, n) - 1
            new, held = update(
                mean_s, norm_v[slot, :, whole : whole + cols], norm_v[slot, :, whole + cols :]
            )
            compute_norm[:, s * cols : (s + 1) * cols] = new.astype(jnp.bfloat16)

    def drain(c, carry):
        for way in range(2):
            for d in range(1, n):

                @pl.when(ahead(way, d))
                def _():
                    sum_copy(way, c, either(way, d)).wait_send()

            for d in range(n):
                s = either(1 - way, d)

                @pl.when(jnp.logical_and(jnp.logical_and(s >= 0, s < n), ahead(way, 1)))
                def _():
                    share_copy(way, c, s).wait_send()

        return carry

    lax.fori_loop(0, count, drain, 0)
    for copy in outs + sum(gathered, []):
        copy.wait()


def line(n, partials, masters, memories, partial_norm, master_norm, memory_norm):
    T, halves = MATRICES, HALVES
    rows, cols = masters[0].shape
    part = rows // halves
    count = T * halves
    whole = partial_norm.shape[1]
    norm_in = jnp.concatenate(
        [partial_norm.astype(jnp.float32), master_norm[None], memory_norm[None]], axis=1
    )
    f32, bf16 = jnp.float32, jnp.bfloat16
    anywhere = pl.BlockSpec(memory_space=pl.ANY)
    inside = pl.BlockSpec(memory_space=pltpu.VMEM)
    share = jax.ShapeDtypeStruct((rows, cols), f32)
    dma = pltpu.SemaphoreType.DMA
    out = pl.pallas_call(
        functools.partial(kernel, n, halves),
        out_shape=[jax.ShapeDtypeStruct(p.shape, bf16) for p in partials]
        + [share] * (2 * T)
        + [jax.ShapeDtypeStruct((1, whole), bf16)]
        + [jax.ShapeDtypeStruct((1, cols), f32)] * 2,
        in_specs=[anywhere] * (3 * T) + [inside],
        out_specs=[anywhere] * (3 * T) + [inside] * 3,
        scratch_shapes=[
            pltpu.VMEM((T, n * rows, cols), bf16),
            pltpu.VMEM((T, rows, cols), f32),
            pltpu.VMEM((T, rows, cols), f32),
            pltpu.VMEM((2, count, n, part, cols), LINK),
            pltpu.VMEM((2, count, n, part, cols), LINK),
            pltpu.VMEM((part, cols), f32),
            pltpu.VMEM((T, rows, cols), f32),
            pltpu.VMEM((T, rows, cols), f32),
            pltpu.VMEM((T, n * rows, cols), bf16),
            pltpu.VMEM((n - 1, 1, whole + 2 * cols), f32),
            dma((T, n)),
            dma((2, T)),
            dma((2, count, n)),
            dma((2, count, n)),
            dma((2, count, n)),
            dma((2, count, n)),
            dma((n - 1,)),
            dma((n - 1,)),
            dma((2, T)),
            dma((T, n)),
        ],
        compiler_params=pltpu.CompilerParams(collective_id=0, has_side_effects=True),
        name="line_step",
    )(*partials, *masters, *memories, norm_in)
    compute, stepped, state = out[:T], out[T : 2 * T], out[2 * T : 3 * T]
    compute_norm, stepped_norm, state_norm = out[3 * T :]
    return (*compute, compute_norm[0], *stepped, stepped_norm[0], *state, state_norm[0])


def plain(n, partials, masters, memories, partial_norm, master_norm, memory_norm):
    rate = n ** (-0.5)
    axes = (0, 0, 0, 1)
    compute, stepped, state = [], [], []
    for p, master, memory, axis in zip(partials, masters, memories, axes):
        total = lax.psum_scatter(
            p.astype(jnp.float32), "replica", scatter_dimension=axis, tiled=True
        )
        new, held = update(total * rate, master, memory)
        stepped.append(new)
        state.append(held)
    whole = lax.psum(partial_norm[0].astype(jnp.float32), "replica")
    size = master_norm.shape[0]
    mean = lax.dynamic_slice_in_dim(whole, lax.axis_index("replica") * size, size) * rate
    new, held = update(mean, master_norm, memory_norm)
    stepped.append(new)
    state.append(held)
    for new, axis in zip(stepped, axes + (0,)):
        compute.append(lax.all_gather(new.astype(jnp.bfloat16), "replica", axis=axis, tiled=True))
    return (*compute, *stepped, *state)


def body(*args):
    partials = [p[0] for p in args[:4]]
    partial_norm = args[4]
    masters, master_norm = args[5:9], args[9]
    memories, memory_norm = args[10:14], args[14]
    n = lax.axis_size("replica")
    shapes = {m.shape for m in masters}
    rows, cols = masters[0].shape
    fits = (
        1 < n <= 4
        and len(shapes) == 1
        and rows % (32 * HALVES) == 0
        and cols % 128 == 0
        and master_norm.shape[0] == cols
    )
    form = line if fits else plain
    return form(n, partials, masters, memories, partial_norm, master_norm, memory_norm)


def solution(mesh):
    tall = P(("site", "replica"), None, "model")
    share, flat = P(("site", "replica"), "model"), P(("site", "replica"))
    wide = P(("site", "model"), "replica")
    shares = (share, share, share, wide, flat)
    return jax.shard_map(
        body,
        mesh=mesh,
        in_specs=(
            tall,
            tall,
            tall,
            P(("site", "replica"), "model", None),
            P(("site", "replica"), None),
            *shares,
            *shares,
        ),
        out_specs=(
            P("site", "model"),
            P("site", "model"),
            P("site", "model"),
            P(("site", "model"), None),
            P("site"),
            *shares,
            *shares,
        ),
        check_vma=False,
    )
```
